32 devices in a mesh: dp: 2 (over x), tp: 4 (over z), kvp: 4 (over y, core).
Axes of the slice: x: 2, y: 2, z: 4, core: 2. Of those that a mesh axis runs over, the one named last changes fastest.
Arguments:
- x_in: bfloat16 [64, 5120], P('dp'), parts along dimension 0
- ctx_len: int32 [64], P('dp'), parts along dimension 0
- g_attn: bfloat16 [5120], replicated
- g_mlp: bfloat16 [5120], replicated
- w_qkv: bfloat16 [5120, 7168], P(None, 'tp')
- w_o: bfloat16 [5120, 5120], P(('tp', 'kvp'))
- w_gate: bfloat16 [5120, 27648], P(None, ('tp', 'kvp'))
- w_up: bfloat16 [5120, 27648], P(None, ('tp', 'kvp'))
- w_down: bfloat16 [27648, 5120], P(('tp', 'kvp'))
- k_cache: bfloat16 [64, 1024, 8, 128], P('dp', 'kvp', 'tp'), parts along dimension 0
- v_cache: bfloat16 [64, 1024, 8, 128], P('dp', 'kvp', 'tp'), parts along dimension 0
Outputs:
- output 1: bfloat16 [64, 5120], P('dp'), parts along dimension 0
- output 2: bfloat16 [64, 1024, 8, 128], P('dp', 'kvp', 'tp'), parts along dimension 0
- output 3: bfloat16 [64, 1024, 8, 128], P('dp', 'kvp', 'tp'), parts along dimension 0
There are 2 independent parts. The reference program is written for one: setup_inputs(seed, part) draws one part's arguments, and reference() takes and returns one part's arrays. A program takes and returns all parts, laid end to end along the dimension named above; an argument that names none is the same for every part.
All inputs are finite; a program needn't handle non-finite values.
Results may differ from the reference program's by a relative error of at most 0.00833289.
Values sent between devices are 32-bit elements.
A program may use at most 1 GiB of HBM per device.

```python
import jax
import jax.numpy as jnp
from jax import lax

D = 5120
HEADS = 40
KV_HEADS = 8
HEAD = 128
FF = 27648
BATCH = 32
SEQ = 1024
NSEG = 16
GROUP = HEADS // KV_HEADS
ROPE_THETA = 500000.0
EPS = 1e-5
NEG_FILL = -1e30


def rms_norm(values, gain_vec):
    x_f32 = values.astype(jnp.float32)
    inv_rms = lax.rsqrt(jnp.mean(x_f32 * x_f32, axis=-1, keepdims=True) + EPS)
    return (x_f32 * inv_rms * gain_vec.astype(jnp.float32)).astype(jnp.bfloat16)


def rope_tables(ctx_len):
    inv_freq = ROPE_THETA ** (-2.0 * jnp.arange(HEAD // 2, dtype=jnp.float32) / HEAD)
    angles = ctx_len.astype(jnp.float32)[:, None] * inv_freq[None, :]
    return jnp.cos(angles), jnp.sin(angles)


def rotary(vectors, cos_t, sin_t):
    half_dim = vectors.shape[-1] // 2
    first_half = vectors[..., :half_dim]
    second_half = vectors[..., half_dim:]
    return jnp.concatenate([first_half * cos_t - second_half * sin_t, second_half * cos_t + first_half * sin_t], axis=-1)


def setup_inputs(seed: int = 0, part: int = 0) -> dict:
    root_key = jax.random.key(seed)
    shared_keys = jax.random.split(root_key, 7)
    part_keys = jax.random.split(jax.random.fold_in(root_key, part), 7)
    x_in = jax.random.normal(part_keys[0], (BATCH, D), jnp.float32).astype(jnp.bfloat16)
    ctx_len = jax.random.randint(part_keys[1], (BATCH,), SEQ // 4, SEQ, dtype=jnp.int32)
    full_row = jax.random.randint(part_keys[2], (), 0, BATCH, dtype=jnp.int32)
    ctx_len = jnp.where(jnp.arange(BATCH) == full_row, SEQ - 1, ctx_len).astype(jnp.int32)
    g_attn = (1.0 + 0.3 * jax.random.normal(shared_keys[0], (D,), jnp.float32)).astype(jnp.bfloat16)
    g_mlp = (1.0 + 0.3 * jax.random.normal(shared_keys[1], (D,), jnp.float32)).astype(jnp.bfloat16)
    w_qkv = (jax.random.normal(shared_keys[2], (D, KV_HEADS * (GROUP + 2) * HEAD), jnp.float32) * D ** -0.5).astype(jnp.bfloat16)
    w_o = (jax.random.normal(shared_keys[3], (HEADS * HEAD, D), jnp.float32) * (HEADS * HEAD) ** -0.5).astype(jnp.bfloat16)
    w_gate = (jax.random.normal(shared_keys[4], (D, FF), jnp.float32) * D ** -0.5).astype(jnp.bfloat16)
    w_up = (jax.random.normal(shared_keys[5], (D, FF), jnp.float32) * D ** -0.5).astype(jnp.bfloat16)
    w_down = (jax.random.normal(shared_keys[6], (FF, D), jnp.float32) * FF ** -0.5).astype(jnp.bfloat16)
    seg_shape = (BATCH, NSEG, 1, KV_HEADS, HEAD)
    noise_shape = (BATCH, NSEG, SEQ // NSEG, KV_HEADS, HEAD)
    cache_shape = (BATCH, SEQ, KV_HEADS, HEAD)
    k_cache = (jax.random.normal(part_keys[3], noise_shape, jnp.float32) + 0.5 * jax.random.normal(part_keys[4], seg_shape, jnp.float32)).reshape(cache_shape).astype(jnp.bfloat16)
    v_cache = (0.5 * jax.random.normal(part_keys[5], noise_shape, jnp.float32) + 2.0 * jax.random.normal(part_keys[6], seg_shape, jnp.float32)).reshape(cache_shape).astype(jnp.bfloat16)
    return {"x_in": x_in, "ctx_len": ctx_len, "g_attn": g_attn, "g_mlp": g_mlp, "w_qkv": w_qkv, "w_o": w_o, "w_gate": w_gate, "w_up": w_up, "w_down": w_down, "k_cache": k_cache, "v_cache": v_cache}


def reference(x_in, ctx_len, g_attn, g_mlp, w_qkv, w_o, w_gate, w_up, w_down, k_cache, v_cache):
    normed = rms_norm(x_in, g_attn)
    qkv_all = jnp.dot(normed, w_qkv, preferred_element_type=jnp.float32).reshape(BATCH, KV_HEADS, GROUP + 2, HEAD)
    cos_t, sin_t = rope_tables(ctx_len)
    queries = rotary(qkv_all[:, :, :GROUP], cos_t[:, None, None, :], sin_t[:, None, None, :]).astype(jnp.bfloat16)
    key_new = rotary(qkv_all[:, :, GROUP], cos_t[:, None, :], sin_t[:, None, :]).astype(jnp.bfloat16)
    val_new = qkv_all[:, :, GROUP + 1].astype(jnp.bfloat16)
    positions = jnp.arange(SEQ)
    hit_mask = (positions[None, :] == ctx_len[:, None])[:, :, None, None]
    k_out = jnp.where(hit_mask, key_new[:, None], k_cache)
    v_out = jnp.where(hit_mask, val_new[:, None], v_cache)
    score_scale = HEAD ** -0.5

    def one_request(row_args):
        q_row, k_row, v_row, length = row_args
        scores = jnp.einsum("grd,tgd->grt", q_row.astype(jnp.float32), k_row.astype(jnp.float32)) * score_scale
        scores = jnp.where(positions <= length, scores, NEG_FILL)
        row_max = jnp.max(scores, axis=-1, keepdims=True)
        prob_w = jnp.exp(scores - row_max)
        denom_sum = jnp.sum(prob_w, axis=-1)
        numer_acc = jnp.einsum("grt,tgd->grd", prob_w.astype(jnp.bfloat16).astype(jnp.float32), v_row.astype(jnp.float32))
        return (numer_acc / denom_sum[..., None]).reshape(HEADS * HEAD)

    attn_all = lax.map(one_request, (queries, k_out, v_out, ctx_len)).astype(jnp.bfloat16)
    hidden = (x_in.astype(jnp.float32) + jnp.dot(attn_all, w_o, preferred_element_type=jnp.float32)).astype(jnp.bfloat16)
    normed_mlp = rms_norm(hidden, g_mlp)
    gate_pre = jnp.dot(normed_mlp, w_gate, preferred_element_type=jnp.float32)
    up_proj = jnp.dot(normed_mlp, w_up, preferred_element_type=jnp.float32)
    act_out = (jax.nn.silu(gate_pre) * up_proj).astype(jnp.bfloat16)
    x_out = (hidden.astype(jnp.float32) + jnp.dot(act_out, w_down, preferred_element_type=jnp.float32)).astype(jnp.bfloat16)
    return (x_out, k_out, v_out)
```

```python
import functools

import jax
import jax.numpy as jnp
from jax import lax
from jax.experimental import pallas as pl
from jax.experimental.pallas import tpu as pltpu
from jax.sharding import PartitionSpec as P

ROPE_THETA = 500000.0
EPS = 1e-5
NEG_FILL = -1e30
LANES = 128
HALF = 16
MESH = pl.DeviceIdType.MESH
QKV_STEPS = 10
KV_STEPS = 4
CHUNKS = 5
UNITS = 8
F32 = jnp.float32
BF16 = jnp.bfloat16


def rope_rows(ctx_len, head_dim):
    inv_freq = ROPE_THETA ** (-2.0 * jnp.arange(head_dim // 2, dtype=F32) / head_dim)
    angles = ctx_len.astype(F32)[:, None] * inv_freq[None, :]
    cos_t, sin_t = jnp.cos(angles), jnp.sin(angles)
    return jnp.concatenate([cos_t, cos_t], axis=-1), jnp.concatenate([-sin_t, sin_t], axis=-1)


def attention_kernel(
    ctx_ref, x_ref, g_ref, cos_ref, sin_ref, w_hbm, k_hbm, v_hbm,
    acc_ref, ml_ref, k_out, v_out,
    w_buf, k_buf, v_buf, n_buf, c_buf, q_buf, kn_buf, vn_buf, m_buf, l_buf,
    w_sem, k_sem, v_sem, ko_sem, vo_sem,
):
    batch, width = x_ref.shape
    rows_w = width // QKV_STEPS
    rows_kv = batch // KV_STEPS
    block2 = k_buf.shape[1]
    block = block2 // 2
    heads = c_buf.shape[1] // LANES
    group = heads // 2 - 2

    def w_copy(i):
        rows = pl.ds(i * rows_w, rows_w)
        return pltpu.make_async_copy(w_hbm.at[rows, :], w_buf.at[rows, :], w_sem.at[i])

    def kv_copy(i, src, dst, sem):
        rows = pl.ds(i * rows_kv, rows_kv)
        return pltpu.make_async_copy(src.at[rows], dst.at[rows], sem.at[i])

    for i in range(QKV_STEPS):
        w_copy(i).start()
    for i in range(KV_STEPS):
        kv_copy(i, k_hbm, k_buf, k_sem).start()
        kv_copy(i, v_hbm, v_buf, v_sem).start()

    sq = jnp.zeros((batch, LANES), F32)
    for c in range(width // LANES):
        xb = x_ref[:, c * LANES:(c + 1) * LANES].astype(F32)
        sq = sq + xb * xb
    inv = lax.rsqrt(jnp.sum(sq, axis=-1, keepdims=True) / width + EPS)
    for i in range(QKV_STEPS):
        cols = slice(i * rows_w, (i + 1) * rows_w)
        xb = x_ref[:, cols].astype(F32)
        n_buf[i] = (xb * inv * g_ref[:, cols].astype(F32)).astype(BF16)

    c_buf[...] = jnp.zeros_like(c_buf)

    def qkv_step(i, carry):
        w_copy(i).wait()
        rows = pl.ds(pl.multiple_of(i * rows_w, rows_w), rows_w)
        c_buf[...] += jnp.dot(n_buf[i], w_buf[rows, :], preferred_element_type=F32)
        return carry

    lax.fori_loop(0, QKV_STEPS, qkv_step, 0)

    cos_t, sin_t = cos_ref[...], sin_ref[...]

    def rotary(v):
        return v * cos_t + pltpu.roll(v, LANES // 2, 1) * sin_t

    q_buf[...] = jnp.zeros_like(q_buf)
    for g in range(2):
        base = g * (group + 2)
        for r in range(group):
            v = c_buf[:, (base + r) * LANES:(base + r + 1) * LANES]
            h = g * group + r
            q_buf[h * batch:(h + 1) * batch, :] = rotary(v).astype(BF16).astype(F32)
        v = c_buf[:, (base + group) * LANES:(base + group + 1) * LANES]
        kn_buf[g * batch:(g + 1) * batch, :] = rotary(v).astype(BF16).astype(F32)
        v = c_buf[:, (base + group + 1) * LANES:(base + group + 2) * LANES]
        vn_buf[g * batch:(g + 1) * batch, :] = v.astype(BF16).astype(F32)

    off = lax.axis_index("kvp") * block
    scale = LANES ** -0.5
    col = lax.broadcasted_iota(jnp.int32, (16, block2), 1)
    row = lax.broadcasted_iota(jnp.int32, (16, block2), 0)
    own = (col & 1) == (row >= group).astype(jnp.int32)
    pos = jnp.where(own, col >> 1, 1 << 20)
    trow = lax.broadcasted_iota(jnp.int32, (16, LANES), 0)
    lane = lax.broadcasted_iota(jnp.int32, (16, LANES), 1)
    m_buf[...] = jnp.zeros_like(m_buf)
    l_buf[...] = jnp.zeros_like(l_buf)

    def kv_step(i, carry):
        kv_copy(i, k_hbm, k_buf, k_sem).wait()
        kv_copy(i, v_hbm, v_buf, v_sem).wait()
        for u in range(rows_kv):
            b = i * rows_kv + u
            rel = ctx_ref[b] - off
            hit = jnp.logical_and(rel >= 0, rel < block)
            relc = jnp.where(hit, rel, 0)
            first = pl.multiple_of((relc >> 3) * 16, 16)
            sel = (trow >> 1) == jnp.where(hit, relc & 7, 64)
            for buf, new in ((k_buf, kn_buf), (v_buf, vn_buf)):
                new0 = new[pl.ds(b, 1), :]
                new1 = new[pl.ds(batch + b, 1), :]
                tile = buf[b, pl.ds(first, 16), :].astype(F32)
                fresh = jnp.where((trow & 1) == 0, new0, new1)
                buf[b, pl.ds(first, 16), :] = jnp.where(sel, fresh, tile).astype(BF16)
        kv_copy(i, k_buf, k_out, ko_sem).start()
        kv_copy(i, v_buf, v_out, vo_sem).start()
        for u in range(rows_kv):
            b = i * rows_kv + u
            rel = ctx_ref[b] - off
            q = q_buf[pl.ds(b, 16, stride=batch), :].astype(BF16)
            s = lax.dot_general(q, k_buf[b], (((1,), (1,)), ((), ())), preferred_element_type=F32) * scale
            s = jnp.where(pos <= rel, s, NEG_FILL)
            m = jnp.max(s, axis=-1, keepdims=True)
            w = jnp.exp(s - m)
            l = jnp.sum(w, axis=-1, keepdims=True)
            acc_ref[pl.ds(b, 16, stride=batch), :] = jnp.dot(w.astype(BF16), v_buf[b], preferred_element_type=F32)
            m_buf[...] += jnp.where(lane == b, m, 0.0)
            l_buf[...] += jnp.where(lane == b, l, 0.0)
        return carry

    lax.fori_loop(0, KV_STEPS, kv_step, 0)
    stats = jnp.concatenate([m_buf[...], l_buf[...], jnp.zeros((LANES - 32, LANES), F32)], axis=0)
    ml_ref[...] = stats.T[:batch, :]
    for i in range(KV_STEPS):
        kv_copy(i, k_buf, k_out, ko_sem).wait()
        kv_copy(i, v_buf, v_out, vo_sem).wait()


def tail_kernel(
    acc_ref, ml_ref, x_ref, g_ref, wo_hbm, wg_hbm, wu_hbm, wd_hbm,
    out_ref,
    wo_buf, wg_buf, wu_buf, wd_buf, racc, rml, a_buf, part, rc_buf, ry_buf, rz_buf, full, h_buf, n_buf, act,
    wo_sem, wg_sem, wu_sem, wd_sem, sa_sem, ra_sem, sm_sem, rm_sem, sc_sem, rc_sem, sy_sem, ry_sem, sz_sem, rz_sem,
):
    batch, width = x_ref.shape
    ff = act.shape[1]
    tp = lax.axis_index("tp")
    kvp = lax.axis_index("kvp")
    y = kvp // 2
    core = kvp % 2
    odd = core
    kv_peers = (y * 2 + (1 - core), (1 - y) * 2 + core, (1 - y) * 2 + (1 - core))
    z_peers = tuple((tp + d) % 4 for d in (1, 2, 3))

    barrier = pltpu.get_barrier_semaphore()
    for peer in kv_peers:
        pl.semaphore_signal(barrier, inc=1, device_id={"kvp": peer}, device_id_type=MESH)
    for peer in z_peers:
        pl.semaphore_signal(barrier, inc=1, device_id={"tp": peer}, device_id_type=MESH)

    rows_o = wo_hbm.shape[0]
    first = pl.multiple_of(odd * 64, 64)
    wo_copy = pltpu.make_async_copy(wo_hbm, wo_buf.at[pl.ds(first, rows_o), :], wo_sem)
    wo_copy.start()
    gap = pl.multiple_of((1 - odd) * rows_o, 64)
    wo_buf[pl.ds(gap, 64), :] = jnp.zeros((64, width), BF16)

    def stream(src, dst, sem, pieces):
        step = src.shape[0] // pieces
        for i in range(pieces):
            rows = pl.ds(i * step, step)
            pltpu.make_async_copy(src.at[rows, :], dst.at[rows, :], sem).start()

    stream(wg_hbm, wg_buf, wg_sem, 8)
    stream(wu_hbm, wu_buf, wu_sem, 8)
    stream(wd_hbm, wd_buf, wd_sem, 9)

    pl.semaphore_wait(barrier, 6)

    sends = []
    for d, peer in enumerate(kv_peers):
        head0 = (5 * peer) // 2
        for src, dst, ss, rs in (
            (acc_ref.at[pl.ds(head0, 3)], racc.at[d], sa_sem, ra_sem),
            (ml_ref, rml.at[d], sm_sem, rm_sem),
        ):
            copy = pltpu.make_async_remote_copy(
                src, dst, ss.at[d], rs.at[d], device_id={"kvp": peer}, device_id_type=MESH
            )
            copy.start()
            sends.append(copy)
    for copy in sends:
        copy.wait_recv()
    head0 = (5 * kvp) // 2
    lane = lax.broadcasted_iota(jnp.int32, (batch, LANES), 1)
    stats = [ml_ref[...]] + [rml[d] for d in range(3)]
    for i in range(3):
        ms = [jnp.sum(jnp.where(lane == head0 + i, st, 0.0), axis=-1, keepdims=True) for st in stats]
        ls = [jnp.sum(jnp.where(lane == head0 + i + 16, st, 0.0), axis=-1, keepdims=True) for st in stats]
        top = functools.reduce(jnp.maximum, ms)
        ws = [jnp.exp(m - top) for m in ms]
        denom = functools.reduce(jnp.add, [l * w for l, w in zip(ls, ws)])
        accs = [acc_ref[head0 + i]] + [racc[d, i] for d in range(3)]
        numer = functools.reduce(jnp.add, [a * w for a, w in zip(accs, ws)])
        a_buf[:, i * LANES:(i + 1) * LANES] = (numer / denom).astype(BF16)

    def remote(src, dst, ss, rs, device):
        copy = pltpu.make_async_remote_copy(src, dst, ss, rs, device_id=device, device_id_type=MESH)
        copy.start()
        return copy

    core_dev = {"kvp": kv_peers[0]}
    y_dev = {"kvp": kv_peers[1]}

    def all_reduce(ar, produce):
        cs, ys, zs, started = [], [], [], []
        for j in range(CHUNKS):
            produce(j)
            cs.append(remote(part.at[1 - core, j], rc_buf.at[ar, j], sc_sem.at[ar, 0, j], rc_sem.at[ar, 0, j], core_dev))
        for j in range(CHUNKS):
            cs[j].wait_recv()
            part[core, j] += rc_buf[ar, j]
            ys.append(remote(part.at[core, j, pl.ds((1 - y) * 4, 4)], ry_buf.at[ar, j], sy_sem.at[ar, 0, j], ry_sem.at[ar, 0, j], y_dev))
        for j in range(CHUNKS):
            ys[j].wait_recv()
            part[core, j, pl.ds(y * 4, 4)] += ry_buf[ar, j]
            zs.append([
                remote(part.at[core, j, y * 4 + peer], rz_buf.at[ar, j, d], sz_sem.at[ar, 0, j, d], rz_sem.at[ar, 0, j, d], {"tp": peer})
                for d, peer in enumerate(z_peers)
            ])
        gz, gy, gc = [], [], []
        mine = y * 4 + tp
        for j in range(CHUNKS):
            total = part[core, j, mine]
            for d in range(3):
                zs[j][d].wait_recv()
                total = total + rz_buf[ar, j, d]
            full[ar, core, j, mine] = total
            gz.append([
                remote(full.at[ar, core, j, mine], full.at[ar, core, j, mine], sz_sem.at[ar, 1, j, d], rz_sem.at[ar, 1, j, d], {"tp": peer})
                for d, peer in enumerate(z_peers)
            ])
        for j in range(CHUNKS):
            for d in range(3):
                gz[j][d].wait_recv()
            block = full.at[ar, core, j, pl.ds(y * 4, 4)]
            gy.append(remote(block, block, sy_sem.at[ar, 1, j], ry_sem.at[ar, 1, j], y_dev))
        for j in range(CHUNKS):
            gy[j].wait_recv()
            block = full.at[ar, core, j]
            gc.append(remote(block, block, sc_sem.at[ar, 1, j], rc_sem.at[ar, 1, j], core_dev))
        for j in range(CHUNKS):
            gc[j].wait_recv()
        for copy in cs + ys + gy + gc:
            copy.wait_send()
        for copy in [c for group in zs + gz for c in group]:
            copy.wait_send()

    wo_copy.wait()

    def store_part(j, half, res):
        for r in range(2):
            for u in range(res.shape[1] // LANES):
                part[r, j, half + u] = res[r * HALF:(r + 1) * HALF, u * LANES:(u + 1) * LANES]

    def produce_o(j):
        cols = slice(j * UNITS * LANES, (j + 1) * UNITS * LANES)
        store_part(j, 0, jnp.dot(a_buf[...], wo_buf[:, cols], preferred_element_type=F32))

    all_reduce(0, produce_o)

    sq = [jnp.zeros((HALF, LANES), F32) for _ in range(2)]
    for c in range(width // LANES):
        j, u = divmod(c, UNITS)
        for r in range(2):
            rows, cols = slice(r * HALF, (r + 1) * HALF), slice(c * LANES, (c + 1) * LANES)
            h = (x_ref[rows, cols].astype(F32) + full[0, r, j, u]).astype(BF16)
            h_buf[rows, cols] = h
            hf = h.astype(F32)
            sq[r] = sq[r] + hf * hf
    for r in range(2):
        rows = slice(r * HALF, (r + 1) * HALF)
        inv = lax.rsqrt(jnp.sum(sq[r], axis=-1, keepdims=True) / width + EPS)
        for c in range(width // LANES):
            cols = slice(c * LANES, (c + 1) * LANES)
            n_buf[rows, cols] = (h_buf[rows, cols].astype(F32) * inv * g_ref[:, cols].astype(F32)).astype(BF16)

    pltpu.make_async_copy(wg_hbm, wg_buf, wg_sem).wait()
    pltpu.make_async_copy(wu_hbm, wu_buf, wu_sem).wait()

    def mlp_tile(cols):
        gate = jnp.dot(n_buf[...], wg_buf[:, cols], preferred_element_type=F32)
        up = jnp.dot(n_buf[...], wu_buf[:, cols], preferred_element_type=F32)
        act[:, cols] = (jax.nn.silu(gate) * up).astype(BF16)

    tiles = ff // 256

    def mlp_step(i, carry):
        mlp_tile(pl.ds(pl.multiple_of(i * 256, 256), 256))
        return carry

    lax.fori_loop(0, tiles, mlp_step, 0)
    if ff % 256:
        mlp_tile(slice(tiles * 256, ff))

    pltpu.make_async_copy(wd_hbm, wd_buf, wd_sem).wait()

    def produce_down(j):
        for half in range(2):
            cols = slice((2 * j + half) * 512, (2 * j + half + 1) * 512)
            store_part(j, half * 4, jnp.dot(act[...], wd_buf[:, cols], preferred_element_type=F32))

    all_reduce(1, produce_down)

    for c in range(width // LANES):
        j, u = divmod(c, UNITS)
        for r in range(2):
            rows, cols = slice(r * HALF, (r + 1) * HALF), slice(c * LANES, (c + 1) * LANES)
            out_ref[rows, cols] = (h_buf[rows, cols].astype(F32) + full[1, r, j, u]).astype(BF16)
    for copy in sends:
        copy.wait_send()


def vmem():
    return pl.BlockSpec(memory_space=pltpu.VMEM)


def anywhere():
    return pl.BlockSpec(memory_space=pl.ANY)


def attention_call(x_in, ctx_len, g_attn, w_qkv, k_cache, v_cache):
    batch, width = x_in.shape
    block, kv_local, head_dim = k_cache.shape[1:]
    cols = w_qkv.shape[1]
    cos_t, sin_t = rope_rows(ctx_len, head_dim)
    flat = (batch, block * kv_local, head_dim)
    dma = pltpu.SemaphoreType.DMA
    acc, ml, k_out, v_out = pl.pallas_call(
        attention_kernel,
        name="attention",
        out_shape=(
            jax.ShapeDtypeStruct((16 * batch, head_dim), F32),
            jax.ShapeDtypeStruct((batch, LANES), F32),
            jax.ShapeDtypeStruct(flat, BF16),
            jax.ShapeDtypeStruct(flat, BF16),
        ),
        in_specs=[pl.BlockSpec(memory_space=pltpu.SMEM)] + [vmem()] * 4 + [anywhere()] * 3,
        out_specs=(vmem(), vmem(), anywhere(), anywhere()),
        scratch_shapes=[
            pltpu.VMEM((width, cols), BF16),
            pltpu.VMEM(flat, BF16),
            pltpu.VMEM(flat, BF16),
            pltpu.VMEM((QKV_STEPS, batch, width // QKV_STEPS), BF16),
            pltpu.VMEM((batch, cols), F32),
            pltpu.VMEM((16 * batch, head_dim), F32),
            pltpu.VMEM((2 * batch, head_dim), F32),
            pltpu.VMEM((2 * batch, head_dim), F32),
            pltpu.VMEM((16, LANES), F32),
            pltpu.VMEM((16, LANES), F32),
            dma((QKV_STEPS,)),
            dma((KV_STEPS,)),
            dma((KV_STEPS,)),
            dma((KV_STEPS,)),
            dma((KV_STEPS,)),
        ],
        compiler_params=pltpu.CompilerParams(vmem_limit_bytes=60 * 1024 * 1024),
        cost_estimate=pl.CostEstimate(flops=2 * batch * width * cols, bytes_accessed=36 << 20, transcendentals=1 << 19),
    )(ctx_len, x_in, g_attn.reshape(1, width), cos_t, sin_t, w_qkv, k_cache.reshape(flat), v_cache.reshape(flat))
    return acc.reshape(16, batch, head_dim), ml, k_out.reshape(k_cache.shape), v_out.reshape(v_cache.shape)


def tail_call(acc, ml, x_in, g_mlp, w_o, w_gate, w_up, w_down):
    batch, width = x_in.shape
    ff = w_gate.shape[1]
    dma = pltpu.SemaphoreType.DMA
    unit = (HALF, LANES)
    return pl.pallas_call(
        tail_kernel,
        name="tail",
        out_shape=jax.ShapeDtypeStruct((batch, width), BF16),
        in_specs=[vmem()] * 4 + [anywhere()] * 4,
        out_specs=vmem(),
        scratch_shapes=[
            pltpu.VMEM((w_o.shape[0] + 64, width), BF16),
            pltpu.VMEM((width, ff), BF16),
            pltpu.VMEM((width, ff), BF16),
            pltpu.VMEM((ff, width), BF16),
            pltpu.VMEM((3, 3, batch, LANES), F32),
            pltpu.VMEM((3, batch, LANES), F32),
            pltpu.VMEM((batch, 3 * LANES), BF16),
            pltpu.VMEM((2, CHUNKS, UNITS) + unit, F32),
            pltpu.VMEM((2, CHUNKS, UNITS) + unit, F32),
            pltpu.VMEM((2, CHUNKS, 4) + unit, F32),
            pltpu.VMEM((2, CHUNKS, 3) + unit, F32),
            pltpu.VMEM((2, 2, CHUNKS, UNITS) + unit, F32),
            pltpu.VMEM((batch, width), BF16),
            pltpu.VMEM((batch, width), BF16),
            pltpu.VMEM((batch, ff), BF16),
            dma(()), dma(()), dma(()), dma(()),
            dma((3,)), dma((3,)), dma((3,)), dma((3,)),
            dma((2, 2, CHUNKS)), dma((2, 2, CHUNKS)),
            dma((2, 2, CHUNKS)), dma((2, 2, CHUNKS)),
            dma((2, 2, CHUNKS, 3)), dma((2, 2, CHUNKS, 3)),
        ],
        compiler_params=pltpu.CompilerParams(
            collective_id=0, has_side_effects=True, vmem_limit_bytes=67_043_328
        ),
        cost_estimate=pl.CostEstimate(flops=6 * batch * width * ff, bytes_accessed=58 << 20, transcendentals=1 << 17),
    )(acc, ml, x_in, g_mlp.reshape(1, width), w_o, w_gate, w_up, w_down)


def solution(mesh):
    x_spec = P("dp", None)
    cache_spec = P("dp", "kvp", "tp", None)
    model_axes = ("tp", "kvp")

    def layer_step(x_in, ctx_len, g_attn, g_mlp, w_qkv, w_o, w_gate, w_up, w_down, k_cache, v_cache):
        acc, ml, k_out, v_out = attention_call(x_in, ctx_len, g_attn, w_qkv, k_cache, v_cache)
        x_out = tail_call(acc, ml, x_in, g_mlp, w_o, w_gate, w_up, w_down)
        return x_out, k_out, v_out

    in_specs = (x_spec, P("dp"), P(None), P(None), P(None, "tp"), P(model_axes, None), P(None, model_axes), P(None, model_axes), P(model_axes, None), cache_spec, cache_spec)
    return jax.shard_map(layer_step, mesh=mesh, in_specs=in_specs, out_specs=(x_spec, cache_spec, cache_spec), check_vma=False)
```

```python
import functools

import jax
import jax.numpy as jnp
from jax import lax
from jax.experimental import pallas as pl
from jax.experimental.pallas import tpu as pltpu
from jax.sharding import PartitionSpec as P

ROPE_THETA = 500000.0
EPS = 1e-5
NEG_FILL = -1e30
LANES = 128
HALF = 16
MESH = pl.DeviceIdType.MESH
QKV_STEPS = 10
KV_STEPS = 4
CHUNKS = 5
GROUPS = ((0, 3), (3, 5))
UNITS = 8
F32 = jnp.float32
BF16 = jnp.bfloat16


def rope_rows(ctx_len, head_dim):
    half_dim = head_dim // 2
    lane = jnp.arange(head_dim)
    pair = (lane % half_dim).astype(F32)
    inv_freq = ROPE_THETA ** (-2.0 * pair / head_dim)
    angles = ctx_len[:, None].astype(F32) * inv_freq[None, :]
    sign = jnp.where(lane < half_dim, -1.0, 1.0)
    return jnp.cos(angles), jnp.sin(angles) * sign[None, :]


def attention_kernel(
    ctx_ref, x_ref, g_ref, cos_ref, sin_ref, w_hbm, k_hbm, v_hbm,
    acc_ref, ml_ref, k_out, v_out,
    w_buf, k_buf, v_buf, n_buf, c_buf, q_buf, kn_buf, vn_buf,
    w_sem, k_sem, v_sem, ko_sem, vo_sem,
):
    batch, width = x_ref.shape
    rows_w = width // QKV_STEPS
    rows_kv = batch // KV_STEPS
    block2 = k_buf.shape[1]
    block = block2 // 2
    heads = c_buf.shape[1] // LANES
    group = heads // 2 - 2

    def w_copy(i):
        rows = pl.ds(i * rows_w, rows_w)
        return pltpu.make_async_copy(w_hbm.at[rows, :], w_buf.at[rows, :], w_sem.at[i])

    def kv_copy(i, src, dst, sem):
        rows = pl.ds(i * rows_kv, rows_kv)
        return pltpu.make_async_copy(src.at[rows], dst.at[rows], sem.at[i])

    for i in range(QKV_STEPS):
        w_copy(i).start()
    for i in range(KV_STEPS):
        kv_copy(i, k_hbm, k_buf, k_sem).start()
        kv_copy(i, v_hbm, v_buf, v_sem).start()

    sq = jnp.zeros((batch, LANES), F32)
    for c in range(width // LANES):
        xb = x_ref[:, c * LANES:(c + 1) * LANES].astype(F32)
        sq = sq + xb * xb
    inv = lax.rsqrt(jnp.sum(sq, axis=-1, keepdims=True) / width + EPS)
    for i in range(QKV_STEPS):
        cols = slice(i * rows_w, (i + 1) * rows_w)
        xb = x_ref[:, cols].astype(F32)
        n_buf[i] = (xb * inv * g_ref[cols].astype(F32)[None, :]).astype(BF16)

    c_buf[...] = jnp.zeros_like(c_buf)

    def qkv_step(i, carry):
        w_copy(i).wait()
        rows = pl.ds(pl.multiple_of(i * rows_w, rows_w), rows_w)
        c_buf[...] += jnp.dot(n_buf[i], w_buf[rows, :], preferred_element_type=F32)
        return carry

    lax.fori_loop(0, QKV_STEPS, qkv_step, 0)

    cos_t, sin_t = cos_ref[...], sin_ref[...]

    def rotary(v):
        return v * cos_t + pltpu.roll(v, LANES // 2, 1) * sin_t

    q_buf[...] = jnp.zeros_like(q_buf)
    for g in range(2):
        base = g * (group + 2)
        for r in range(group):
            v = c_buf[:, (base + r) * LANES:(base + r + 1) * LANES]
            h = g * group + r
            q_buf[h * batch:(h + 1) * batch, :] = rotary(v).astype(BF16).astype(F32)
        v = c_buf[:, (base + group) * LANES:(base + group + 1) * LANES]
        kn_buf[g * batch:(g + 1) * batch, :] = rotary(v).astype(BF16).astype(F32)
        v = c_buf[:, (base + group + 1) * LANES:(base + group + 2) * LANES]
        vn_buf[g * batch:(g + 1) * batch, :] = v.astype(BF16).astype(F32)

    off = lax.axis_index("kvp") * block
    scale = LANES ** -0.5
    col = lax.broadcasted_iota(jnp.int32, (16, block2), 1)
    row = lax.broadcasted_iota(jnp.int32, (16, block2), 0)
    own = (col & 1) == (row >= group).astype(jnp.int32)
    pos = jnp.where(own, col >> 1, 1 << 20)
    trow = lax.broadcasted_iota(jnp.int32, (16, LANES), 0)
    lane = lax.broadcasted_iota(jnp.int32, (16, LANES), 1)
    def kv_step(i, carry):
        m_all, l_all = carry
        kv_copy(i, k_hbm, k_buf, k_sem).wait()
        kv_copy(i, v_hbm, v_buf, v_sem).wait()
        rels = [ctx_ref[i * rows_kv + u] - off for u in range(rows_kv)]
        fresh = []
        for u in range(rows_kv):
            b = i * rows_kv + u
            hit = jnp.logical_and(rels[u] >= 0, rels[u] < block)
            relc = jnp.where(hit, rels[u], 0)
            first = pl.multiple_of((relc >> 3) * 16, 16)
            sel = (trow >> 1) == jnp.where(hit, relc & 7, 64)
            for buf, new in ((k_buf, kn_buf), (v_buf, vn_buf)):
                new0 = new[pl.ds(b, 1), :]
                new1 = new[pl.ds(batch + b, 1), :]
                tile = buf[b, pl.ds(first, 16), :].astype(F32)
                row_pair = jnp.where((trow & 1) == 0, new0, new1)
                fresh.append((buf, b, first, jnp.where(sel, row_pair, tile).astype(BF16)))
        for buf, b, first, tile in fresh:
            buf[b, pl.ds(first, 16), :] = tile
        kv_copy(i, k_buf, k_out, ko_sem).start()
        kv_copy(i, v_buf, v_out, vo_sem).start()
        results = []
        qs = [q_buf[pl.ds(i * rows_kv + u, 16, stride=batch), :].astype(BF16) for u in range(rows_kv)]
        scores = [
            lax.dot_general(qs[u], k_buf[i * rows_kv + u], (((1,), (1,)), ((), ())), preferred_element_type=F32)
            for u in range(rows_kv)
        ]
        for u in range(rows_kv):
            b = i * rows_kv + u
            s = jnp.where(pos <= rels[u], scores[u] * scale, NEG_FILL)
            m = jnp.max(s, axis=-1, keepdims=True)
            w = jnp.exp(s - m)
            l = jnp.sum(w, axis=-1, keepdims=True)
            m_all = m_all + jnp.where(lane == b, m, 0.0)
            l_all = l_all + jnp.where(lane == b, l, 0.0)
            results.append(jnp.dot(w.astype(BF16), v_buf[b], preferred_element_type=F32))
        for u in range(rows_kv):
            acc_ref[pl.ds(i * rows_kv + u, 16, stride=batch), :] = results[u]
        return m_all, l_all

    zero = jnp.zeros((16, LANES), F32)
    m_all, l_all = lax.fori_loop(0, KV_STEPS, kv_step, (zero, zero))
    stats = jnp.concatenate([m_all, l_all, jnp.zeros((LANES - 32, LANES), F32)], axis=0)
    ml_ref[...] = stats.T[:batch, :]
    for i in range(KV_STEPS):
        kv_copy(i, k_buf, k_out, ko_sem).wait()
        kv_copy(i, v_buf, v_out, vo_sem).wait()


def tail_kernel(
    acc_ref, ml_ref, x_ref, g_ref, wo_hbm, wg_hbm, wu_hbm, wd_hbm,
    out_ref,
    wo_buf, wg_buf, wu_buf, wd_buf, racc, rml, a_buf, part, rc_buf, ry_buf, rz_buf, full, h_buf, n_buf, act,
    wo_sem, wg_sem, wu_sem, wd_sem, sa_sem, ra_sem, sm_sem, rm_sem, sc_sem, rc_sem, sy_sem, ry_sem, sz_sem, rz_sem,
):
    batch, width = x_ref.shape
    ff = act.shape[1]
    tp = lax.axis_index("tp")
    kvp = lax.axis_index("kvp")
    y = kvp // 2
    core = kvp % 2
    odd = core
    kv_peers = (y * 2 + (1 - core), (1 - y) * 2 + core, (1 - y) * 2 + (1 - core))
    z_peers = tuple((tp + d) % 4 for d in (1, 2, 3))

    barrier = pltpu.get_barrier_semaphore()
    for peer in kv_peers:
        pl.semaphore_signal(barrier, inc=1, device_id={"kvp": peer}, device_id_type=MESH)
    for peer in z_peers:
        pl.semaphore_signal(barrier, inc=1, device_id={"tp": peer}, device_id_type=MESH)

    rows_o = wo_hbm.shape[0]
    first = pl.multiple_of(odd * 64, 64)
    wo_copy = pltpu.make_async_copy(wo_hbm, wo_buf.at[pl.ds(first, rows_o), :], wo_sem)
    wo_copy.start()
    gap = pl.multiple_of((1 - odd) * rows_o, 64)
    wo_buf[pl.ds(gap, 64), :] = jnp.zeros((64, width), BF16)

    def stream(src, dst, sem, pieces):
        step = src.shape[0] // pieces
        for i in range(pieces):
            rows = pl.ds(i * step, step)
            pltpu.make_async_copy(src.at[rows, :], dst.at[rows, :], sem).start()

    stream(wg_hbm, wg_buf, wg_sem, 9)
    stream(wu_hbm, wu_buf, wu_sem, 9)
    stream(wd_hbm, wd_buf, wd_sem, 9)

    pl.semaphore_wait(barrier, 6)

    sends = []
    for d, peer in enumerate(kv_peers):
        head0 = (5 * peer) // 2
        for src, dst, ss, rs in (
            (acc_ref.at[pl.ds(head0, 3)], racc.at[d], sa_sem, ra_sem),
            (ml_ref, rml.at[d], sm_sem, rm_sem),
        ):
            copy = pltpu.make_async_remote_copy(
                src, dst, ss.at[d], rs.at[d], device_id={"kvp": peer}, device_id_type=MESH
            )
            copy.start()
            sends.append(copy)
    for copy in sends:
        copy.wait_recv()
    head0 = (5 * kvp) // 2
    lane = lax.broadcasted_iota(jnp.int32, (batch, LANES), 1)
    stats = [ml_ref[...]] + [rml[d] for d in range(3)]
    for i in range(3):
        ms = [jnp.sum(jnp.where(lane == head0 + i, st, 0.0), axis=-1, keepdims=True) for st in stats]
        ls = [jnp.sum(jnp.where(lane == head0 + i + 16, st, 0.0), axis=-1, keepdims=True) for st in stats]
        top = functools.reduce(jnp.maximum, ms)
        ws = [jnp.exp(m - top) for m in ms]
        denom = functools.reduce(jnp.add, [l * w for l, w in zip(ls, ws)])
        accs = [acc_ref[head0 + i]] + [racc[d, i] for d in range(3)]
        numer = functools.reduce(jnp.add, [a * w for a, w in zip(accs, ws)])
        a_buf[:, i * LANES:(i + 1) * LANES] = (numer / denom).astype(BF16)

    def remote(src, dst, ss, rs, device):
        copy = pltpu.make_async_remote_copy(src, dst, ss, rs, device_id=device, device_id_type=MESH)
        copy.start()
        return copy

    core_dev = {"kvp": kv_peers[0]}
    y_dev = {"kvp": kv_peers[1]}

    def all_reduce(ar, produce):
        cs, ys, zs, started = [], [], [], []
        for j in range(CHUNKS):
            produce(j)
            cs.append(remote(part.at[1 - core, j], rc_buf.at[ar, j], sc_sem.at[ar, 0, j], rc_sem.at[ar, 0, j], core_dev))
        for j0, j1 in GROUPS:
            chunks = pl.ds(j0, j1 - j0)
            for j in range(j0, j1):
                cs[j].wait_recv()
                part[core, j] += rc_buf[ar, j]
            ys.append(remote(part.at[core, chunks, pl.ds((1 - y) * 4, 4)], ry_buf.at[ar, chunks], sy_sem.at[ar, 0, j0], ry_sem.at[ar, 0, j0], y_dev))
        for i, (j0, j1) in enumerate(GROUPS):
            chunks = pl.ds(j0, j1 - j0)
            ys[i].wait_recv()
            for j in range(j0, j1):
                part[core, j, pl.ds(y * 4, 4)] += ry_buf[ar, j]
            zs.append([
                remote(part.at[core, chunks, y * 4 + peer], rz_buf.at[ar, d, chunks], sz_sem.at[ar, 0, j0, d], rz_sem.at[ar, 0, j0, d], {"tp": peer})
                for d, peer in enumerate(z_peers)
            ])
        gz, gy, gc = [], [], []
        mine = y * 4 + tp
        for i, (j0, j1) in enumerate(GROUPS):
            chunks = pl.ds(j0, j1 - j0)
            for d in range(3):
                zs[i][d].wait_recv()
            for j in range(j0, j1):
                full[ar, core, j, mine] = part[core, j, mine] + rz_buf[ar, 0, j] + rz_buf[ar, 1, j] + rz_buf[ar, 2, j]
            block = full.at[ar, core, chunks, mine]
            gz.append([
                remote(block, block, sz_sem.at[ar, 1, j0, d], rz_sem.at[ar, 1, j0, d], {"tp": peer})
                for d, peer in enumerate(z_peers)
            ])
        for i, (j0, j1) in enumerate(GROUPS):
            for d in range(3):
                gz[i][d].wait_recv()
            block = full.at[ar, core, pl.ds(j0, j1 - j0), pl.ds(y * 4, 4)]
            gy.append(remote(block, block, sy_sem.at[ar, 1, j0], ry_sem.at[ar, 1, j0], y_dev))
        for i, (j0, j1) in enumerate(GROUPS):
            gy[i].wait_recv()
            block = full.at[ar, core, pl.ds(j0, j1 - j0)]
            gc.append(remote(block, block, sc_sem.at[ar, 1, j0], rc_sem.at[ar, 1, j0], core_dev))
        for copy in gc:
            copy.wait_recv()
        for copy in cs + ys + gy + gc:
            copy.wait_send()
        for copy in [c for group in zs + gz for c in group]:
            copy.wait_send()

    wo_copy.wait()

    def store_part(j, half, res):
        for r in range(2):
            for u in range(res.shape[1] // LANES):
                part[r, j, half + u] = res[r * HALF:(r + 1) * HALF, u * LANES:(u + 1) * LANES]

    def produce_o(j):
        cols = slice(j * UNITS * LANES, (j + 1) * UNITS * LANES)
        store_part(j, 0, jnp.dot(a_buf[...], wo_buf[:, cols], preferred_element_type=F32))

    all_reduce(0, produce_o)

    sq = [jnp.zeros((HALF, LANES), F32) for _ in range(2)]
    for c in range(width // LANES):
        j, u = divmod(c, UNITS)
        for r in range(2):
            rows, cols = slice(r * HALF, (r + 1) * HALF), slice(c * LANES, (c + 1) * LANES)
            h = (x_ref[rows, cols].astype(F32) + full[0, r, j, u]).astype(BF16)
            h_buf[rows, cols] = h
            hf = h.astype(F32)
            sq[r] = sq[r] + hf * hf
    for r in range(2):
        rows = slice(r * HALF, (r + 1) * HALF)
        inv = lax.rsqrt(jnp.sum(sq[r], axis=-1, keepdims=True) / width + EPS)
        for c in range(width // LANES):
            cols = slice(c * LANES, (c + 1) * LANES)
            n_buf[rows, cols] = (h_buf[rows, cols].astype(F32) * inv * g_ref[cols].astype(F32)[None, :]).astype(BF16)

    pltpu.make_async_copy(wg_hbm, wg_buf, wg_sem).wait()
    pltpu.make_async_copy(wu_hbm, wu_buf, wu_sem).wait()

    def dot_t(a, b):
        return lax.dot_general(a, b, (((1,), (1,)), ((), ())), preferred_element_type=F32)

    def mlp_tile(cols):
        gate = dot_t(n_buf[...], wg_buf[cols, :])
        up = dot_t(n_buf[...], wu_buf[cols, :])
        act[:, cols] = (jax.nn.silu(gate) * up).astype(BF16)

    tiles = ff // 256

    def mlp_step(i, carry):
        mlp_tile(pl.ds(pl.multiple_of(i * 256, 256), 256))
        return carry

    lax.fori_loop(0, tiles, mlp_step, 0)
    if ff % 256:
        mlp_tile(slice(tiles * 256, ff))

    pltpu.make_async_copy(wd_hbm, wd_buf, wd_sem).wait()

    def produce_down(j):
        for half in range(2):
            cols = slice((2 * j + half) * 512, (2 * j + half + 1) * 512)
            store_part(j, half * 4, jnp.dot(act[...], wd_buf[:, cols], preferred_element_type=F32))

    all_reduce(1, produce_down)

    for c in range(width // LANES):
        j, u = divmod(c, UNITS)
        for r in range(2):
            rows, cols = slice(r * HALF, (r + 1) * HALF), slice(c * LANES, (c + 1) * LANES)
            out_ref[rows, cols] = (h_buf[rows, cols].astype(F32) + full[1, r, j, u]).astype(BF16)
    for copy in sends:
        copy.wait_send()


def vmem():
    return pl.BlockSpec(memory_space=pltpu.VMEM)


def anywhere():
    return pl.BlockSpec(memory_space=pl.ANY)


def attention_call(x_in, ctx_len, g_attn, w_qkv, k_cache, v_cache):
    batch, width = x_in.shape
    block, kv_local, head_dim = k_cache.shape[1:]
    cols = w_qkv.shape[1]
    cos_t, sin_t = rope_rows(ctx_len, head_dim)
    flat = (batch, block * kv_local, head_dim)
    dma = pltpu.SemaphoreType.DMA
    acc, ml, k_out, v_out = pl.pallas_call(
        attention_kernel,
        name="attention",
        out_shape=(
            jax.ShapeDtypeStruct((16 * batch, head_dim), F32),
            jax.ShapeDtypeStruct((batch, LANES), F32),
            jax.ShapeDtypeStruct(flat, BF16),
            jax.ShapeDtypeStruct(flat, BF16),
        ),
        in_specs=[pl.BlockSpec(memory_space=pltpu.SMEM)] + [vmem()] * 4 + [anywhere()] * 3,
        out_specs=(vmem(), vmem(), anywhere(), anywhere()),
        scratch_shapes=[
            pltpu.VMEM((width, cols), BF16),
            pltpu.VMEM(flat, BF16),
            pltpu.VMEM(flat, BF16),
            pltpu.VMEM((QKV_STEPS, batch, width // QKV_STEPS), BF16),
            pltpu.VMEM((batch, cols), F32),
            pltpu.VMEM((16 * batch, head_dim), F32),
            pltpu.VMEM((2 * batch, head_dim), F32),
            pltpu.VMEM((2 * batch, head_dim), F32),
            dma((QKV_STEPS,)),
            dma((KV_STEPS,)),
            dma((KV_STEPS,)),
            dma((KV_STEPS,)),
            dma((KV_STEPS,)),
        ],
        compiler_params=pltpu.CompilerParams(vmem_limit_bytes=60 * 1024 * 1024),
        cost_estimate=pl.CostEstimate(flops=2 * batch * width * cols, bytes_accessed=36 << 20, transcendentals=1 << 19),
    )(ctx_len, x_in, g_attn, cos_t, sin_t, w_qkv, k_cache.reshape(flat), v_cache.reshape(flat))
    return acc.reshape(16, batch, head_dim), ml, k_out.reshape(k_cache.shape), v_out.reshape(v_cache.shape)


def tail_call(acc, ml, x_in, g_mlp, w_o, w_gate, w_up, w_down):
    batch, width = x_in.shape
    ff = w_gate.shape[1]
    dma = pltpu.SemaphoreType.DMA
    unit = (HALF, LANES)
    return pl.pallas_call(
        tail_kernel,
        name="tail",
        out_shape=jax.ShapeDtypeStruct((batch, width), BF16),
        in_specs=[vmem()] * 4 + [anywhere()] * 4,
        out_specs=vmem(),
        scratch_shapes=[
            pltpu.VMEM((w_o.shape[0] + 64, width), BF16),
            pltpu.VMEM((ff, width), BF16),
            pltpu.VMEM((ff, width), BF16),
            pltpu.VMEM((ff, width), BF16),
            pltpu.VMEM((3, 3, batch, LANES), F32),
            pltpu.VMEM((3, batch, LANES), F32),
            pltpu.VMEM((batch, 3 * LANES), BF16),
            pltpu.VMEM((2, CHUNKS, UNITS) + unit, F32),
            pltpu.VMEM((2, CHUNKS, UNITS) + unit, F32),
            pltpu.VMEM((2, CHUNKS, 4) + unit, F32),
            pltpu.VMEM((2, 3, CHUNKS) + unit, F32),
            pltpu.VMEM((2, 2, CHUNKS, UNITS) + unit, F32),
            pltpu.VMEM((batch, width), BF16),
            pltpu.VMEM((batch, width), BF16),
            pltpu.VMEM((batch, ff), BF16),
            dma(()), dma(()), dma(()), dma(()),
            dma((3,)), dma((3,)), dma((3,)), dma((3,)),
            dma((2, 2, CHUNKS)), dma((2, 2, CHUNKS)),
            dma((2, 2, CHUNKS)), dma((2, 2, CHUNKS)),
            dma((2, 2, CHUNKS, 3)), dma((2, 2, CHUNKS, 3)),
        ],
        compiler_params=pltpu.CompilerParams(
            collective_id=0, has_side_effects=True, vmem_limit_bytes=67_043_328
        ),
        cost_estimate=pl.CostEstimate(flops=6 * batch * width * ff, bytes_accessed=58 << 20, transcendentals=1 << 17),
    )(acc, ml, x_in, g_mlp, w_o, w_gate.T, w_up.T, w_down)


def solution(mesh):
    x_spec = P("dp", None)
    cache_spec = P("dp", "kvp", "tp", None)
    model_axes = ("tp", "kvp")

    def layer_step(x_in, ctx_len, g_attn, g_mlp, w_qkv, w_o, w_gate, w_up, w_down, k_cache, v_cache):
        acc, ml, k_out, v_out = attention_call(x_in, ctx_len, g_attn, w_qkv, k_cache, v_cache)
        x_out = tail_call(acc, ml, x_in, g_mlp, w_o, w_gate, w_up, w_down)
        return x_out, k_out, v_out

    in_specs = (x_spec, P("dp"), P(None), P(None), P(None, "tp"), P(model_axes, None), P(None, model_axes), P(None, model_axes), P(model_axes, None), cache_spec, cache_spec)
    return jax.shard_map(layer_step, mesh=mesh, in_specs=in_specs, out_specs=(x_spec, cache_spec, cache_spec), check_vma=False)
```

```python
import functools

import jax
import jax.numpy as jnp
from jax import lax
from jax.experimental import pallas as pl
from jax.experimental.pallas import tpu as pltpu
from jax.sharding import PartitionSpec as P

ROPE_THETA = 500000.0
EPS = 1e-5
NEG_FILL = -1e30
LANES = 128
HALF = 16
MESH = pl.DeviceIdType.MESH
QKV_STEPS = 10
PIECES = 9
KV_STEPS = 4
CHUNKS = 5
GROUPS = ((0, 1), (1, 2), (2, 3), (3, 4), (4, 5))
UNITS = 8
F32 = jnp.float32
BF16 = jnp.bfloat16


def rope_rows(ctx_len, head_dim):
    half_dim = head_dim // 2
    lane = jnp.arange(head_dim)
    pair = (lane % half_dim).astype(F32)
    inv_freq = ROPE_THETA ** (-2.0 * pair / head_dim)
    angles = ctx_len[:, None].astype(F32) * inv_freq[None, :]
    sign = jnp.where(lane < half_dim, -1.0, 1.0)
    return jnp.cos(angles), jnp.sin(angles) * sign[None, :]


def attention_kernel(
    ctx_ref, x_ref, g_ref, cos_ref, sin_ref, w_hbm, k_hbm, v_hbm,
    acc_ref, ml_ref, k_out, v_out,
    w_buf, k_buf, v_buf, n_buf, c_buf, q_buf, kn_buf, vn_buf,
    w_sem, k_sem, v_sem, ko_sem, vo_sem,
):
    batch, width = x_ref.shape
    rows_w = width // QKV_STEPS
    rows_kv = batch // KV_STEPS
    block2 = k_buf.shape[1]
    block = block2 // 2
    heads = c_buf.shape[1] // LANES
    group = heads // 2 - 2

    def w_copy(i):
        rows = pl.ds(i * rows_w, rows_w)
        return pltpu.make_async_copy(w_hbm.at[rows, :], w_buf.at[rows, :], w_sem.at[i])

    def kv_copy(i, src, dst, sem):
        rows = pl.ds(i * rows_kv, rows_kv)
        return pltpu.make_async_copy(src.at[rows], dst.at[rows], sem.at[i])

    for i in range(QKV_STEPS):
        w_copy(i).start()
    for i in range(KV_STEPS):
        kv_copy(i, k_hbm, k_buf, k_sem).start()
        kv_copy(i, v_hbm, v_buf, v_sem).start()

    sq = jnp.zeros((batch, LANES), F32)
    for c in range(width // LANES):
        xb = x_ref[:, c * LANES:(c + 1) * LANES].astype(F32)
        sq = sq + xb * xb
    inv = lax.rsqrt(jnp.sum(sq, axis=-1, keepdims=True) / width + EPS)
    for i in range(QKV_STEPS):
        cols = slice(i * rows_w, (i + 1) * rows_w)
        xb = x_ref[:, cols].astype(F32)
        n_buf[i] = (xb * inv * g_ref[cols].astype(F32)[None, :]).astype(BF16)

    c_buf[...] = jnp.zeros_like(c_buf)

    def qkv_step(i, carry):
        w_copy(i).wait()
        rows = pl.ds(pl.multiple_of(i * rows_w, rows_w), rows_w)
        c_buf[...] += jnp.dot(n_buf[i], w_buf[rows, :], preferred_element_type=F32)
        return carry

    lax.fori_loop(0, QKV_STEPS, qkv_step, 0)

    cos_t, sin_t = cos_ref[...], sin_ref[...]

    def rotary(v):
        return v * cos_t + pltpu.roll(v, LANES // 2, 1) * sin_t

    q_buf[...] = jnp.zeros_like(q_buf)
    for g in range(2):
        base = g * (group + 2)
        for r in range(group):
            v = c_buf[:, (base + r) * LANES:(base + r + 1) * LANES]
            h = g * group + r
            q_buf[h * batch:(h + 1) * batch, :] = rotary(v).astype(BF16).astype(F32)
        v = c_buf[:, (base + group) * LANES:(base + group + 1) * LANES]
        kn_buf[g * batch:(g + 1) * batch, :] = rotary(v).astype(BF16).astype(F32)
        v = c_buf[:, (base + group + 1) * LANES:(base + group + 2) * LANES]
        vn_buf[g * batch:(g + 1) * batch, :] = v.astype(BF16).astype(F32)

    off = lax.axis_index("kvp") * block
    scale = LANES ** -0.5
    col = lax.broadcasted_iota(jnp.int32, (16, block2), 1)
    row = lax.broadcasted_iota(jnp.int32, (16, block2), 0)
    own = (col & 1) == (row >= group).astype(jnp.int32)
    pos = jnp.where(own, col >> 1, 1 << 20)
    trow = lax.broadcasted_iota(jnp.int32, (16, LANES), 0)
    lane = lax.broadcasted_iota(jnp.int32, (16, LANES), 1)
    def kv_step(i, carry):
        m_all, l_all = carry
        kv_copy(i, k_hbm, k_buf, k_sem).wait()
        kv_copy(i, v_hbm, v_buf, v_sem).wait()
        rels = [ctx_ref[i * rows_kv + u] - off for u in range(rows_kv)]
        fresh = []
        for u in range(rows_kv):
            b = i * rows_kv + u
            hit = jnp.logical_and(rels[u] >= 0, rels[u] < block)
            relc = jnp.where(hit, rels[u], 0)
            first = pl.multiple_of((relc >> 3) * 16, 16)
            sel = (trow >> 1) == jnp.where(hit, relc & 7, 64)
            for buf, new in ((k_buf, kn_buf), (v_buf, vn_buf)):
                new0 = new[pl.ds(b, 1), :]
                new1 = new[pl.ds(batch + b, 1), :]
                tile = buf[b, pl.ds(first, 16), :].astype(F32)
                row_pair = jnp.where((trow & 1) == 0, new0, new1)
                fresh.append((buf, b, first, jnp.where(sel, row_pair, tile).astype(BF16)))
        for buf, b, first, tile in fresh:
            buf[b, pl.ds(first, 16), :] = tile
        kv_copy(i, k_buf, k_out, ko_sem).start()
        kv_copy(i, v_buf, v_out, vo_sem).start()
        results = []
        qs = [q_buf[pl.ds(i * rows_kv + u, 16, stride=batch), :].astype(BF16) for u in range(rows_kv)]
        scores = [
            lax.dot_general(qs[u], k_buf[i * rows_kv + u], (((1,), (1,)), ((), ())), preferred_element_type=F32)
            for u in range(rows_kv)
        ]
        for u in range(rows_kv):
            b = i * rows_kv + u
            s = jnp.where(pos <= rels[u], scores[u] * scale, NEG_FILL)
            m = jnp.max(s, axis=-1, keepdims=True)
            w = jnp.exp(s - m)
            l = jnp.sum(w, axis=-1, keepdims=True)
            m_all = m_all + jnp.where(lane == b, m, 0.0)
            l_all = l_all + jnp.where(lane == b, l, 0.0)
            results.append(jnp.dot(w.astype(BF16), v_buf[b], preferred_element_type=F32))
        for u in range(rows_kv):
            acc_ref[pl.ds(i * rows_kv + u, 16, stride=batch), :] = results[u]
        return m_all, l_all

    zero = jnp.zeros((16, LANES), F32)
    m_all, l_all = lax.fori_loop(0, KV_STEPS, kv_step, (zero, zero))
    stats = jnp.concatenate([m_all, l_all, jnp.zeros((LANES - 32, LANES), F32)], axis=0)
    ml_ref[...] = stats.T[:batch, :]
    for i in range(KV_STEPS):
        kv_copy(i, k_buf, k_out, ko_sem).wait()
        kv_copy(i, v_buf, v_out, vo_sem).wait()


def tail_kernel(
    acc_ref, ml_ref, x_ref, g_ref, wo_hbm, wg_hbm, wu_hbm, wd_hbm,
    out_ref,
    wo_buf, wg_buf, wu_buf, wd_buf, racc, rml, a_buf, part, rc_buf, ry_buf, rz_buf, full, h_buf, n_buf, act,
    wo_sem, wg_sem, wu_sem, wd_sem, sa_sem, ra_sem, sm_sem, rm_sem, sc_sem, rc_sem, sy_sem, ry_sem, sz_sem, rz_sem,
):
    batch, width = x_ref.shape
    ff = act.shape[1]
    tp = lax.axis_index("tp")
    kvp = lax.axis_index("kvp")
    y = kvp // 2
    core = kvp % 2
    odd = core
    kv_peers = (y * 2 + (1 - core), (1 - y) * 2 + core, (1 - y) * 2 + (1 - core))
    z_peers = tuple((tp + d) % 4 for d in (1, 2, 3))

    barrier = pltpu.get_barrier_semaphore()
    for peer in kv_peers:
        pl.semaphore_signal(barrier, inc=1, device_id={"kvp": peer}, device_id_type=MESH)
    for peer in z_peers:
        pl.semaphore_signal(barrier, inc=1, device_id={"tp": peer}, device_id_type=MESH)

    rows_o = wo_hbm.shape[0]
    first = pl.multiple_of(odd * 64, 64)
    wo_copy = pltpu.make_async_copy(wo_hbm, wo_buf.at[pl.ds(first, rows_o), :], wo_sem)
    wo_copy.start()
    gap = pl.multiple_of((1 - odd) * rows_o, 64)
    wo_buf[pl.ds(gap, 64), :] = jnp.zeros((64, width), BF16)

    pieces = []
    for src, dst, sem in ((wg_hbm, wg_buf, wg_sem), (wu_hbm, wu_buf, wu_sem), (wd_hbm, wd_buf, wd_sem)):
        step = src.shape[0] // PIECES
        for i in range(PIECES):
            pieces.append((src.at[pl.ds(i * step, step), :], dst.at[pl.ds(i * step, step), :], sem))

    def pump(count):
        for _ in range(min(count, len(pieces))):
            pltpu.make_async_copy(*pieces.pop(0)).start()

    pump(2)
    pl.semaphore_wait(barrier, 6)

    sends = []
    for d, peer in enumerate(kv_peers):
        head0 = (5 * peer) // 2
        for src, dst, ss, rs in (
            (acc_ref.at[pl.ds(head0, 3)], racc.at[d], sa_sem, ra_sem),
            (ml_ref, rml.at[d], sm_sem, rm_sem),
        ):
            copy = pltpu.make_async_remote_copy(
                src, dst, ss.at[d], rs.at[d], device_id={"kvp": peer}, device_id_type=MESH
            )
            copy.start()
            sends.append(copy)
    pump(6)
    for copy in sends:
        copy.wait_recv()
    head0 = (5 * kvp) // 2
    lane = lax.broadcasted_iota(jnp.int32, (batch, LANES), 1)
    stats = [ml_ref[...]] + [rml[d] for d in range(3)]
    for i in range(3):
        ms = [jnp.sum(jnp.where(lane == head0 + i, st, 0.0), axis=-1, keepdims=True) for st in stats]
        ls = [jnp.sum(jnp.where(lane == head0 + i + 16, st, 0.0), axis=-1, keepdims=True) for st in stats]
        top = functools.reduce(jnp.maximum, ms)
        ws = [jnp.exp(m - top) for m in ms]
        denom = functools.reduce(jnp.add, [l * w for l, w in zip(ls, ws)])
        accs = [acc_ref[head0 + i]] + [racc[d, i] for d in range(3)]
        numer = functools.reduce(jnp.add, [a * w for a, w in zip(accs, ws)])
        a_buf[:, i * LANES:(i + 1) * LANES] = (numer / denom).astype(BF16)

    def remote(src, dst, ss, rs, device):
        copy = pltpu.make_async_remote_copy(src, dst, ss, rs, device_id=device, device_id_type=MESH)
        copy.start()
        return copy

    core_dev = {"kvp": kv_peers[0]}
    y_dev = {"kvp": kv_peers[1]}

    def all_reduce(ar, produce, lag):
        cs, ys, zs, started = [], [], [], []
        def core_sum(j0, j1):
            chunks = pl.ds(j0, j1 - j0)
            for j in range(j0, j1):
                cs[j].wait_recv()
                part[core, j] += rc_buf[ar, j]
            ys.append(remote(part.at[core, chunks, pl.ds((1 - y) * 4, 4)], ry_buf.at[ar, chunks], sy_sem.at[ar, 0, j0], ry_sem.at[ar, 0, j0], y_dev))

        for j in range(CHUNKS):
            produce(j)
            cs.append(remote(part.at[1 - core, j], rc_buf.at[ar, j], sc_sem.at[ar, 0, j], rc_sem.at[ar, 0, j], core_dev))
            if j - lag >= 0:
                core_sum(*GROUPS[j - lag])
        for j in range(CHUNKS - lag, CHUNKS):
            core_sum(*GROUPS[j])
        pump(3)
        for i, (j0, j1) in enumerate(GROUPS):
            chunks = pl.ds(j0, j1 - j0)
            ys[i].wait_recv()
            for j in range(j0, j1):
                part[core, j, pl.ds(y * 4, 4)] += ry_buf[ar, j]
            zs.append([
                remote(part.at[core, chunks, y * 4 + peer], rz_buf.at[ar, d, chunks], sz_sem.at[ar, 0, j0, d], rz_sem.at[ar, 0, j0, d], {"tp": peer})
                for d, peer in enumerate(z_peers)
            ])
            pump(1)
        gz, gy, gc = [], [], []
        mine = y * 4 + tp
        for i, (j0, j1) in enumerate(GROUPS):
            chunks = pl.ds(j0, j1 - j0)
            for d in range(3):
                zs[i][d].wait_recv()
            for j in range(j0, j1):
                full[ar, core, j, mine] = part[core, j, mine] + rz_buf[ar, 0, j] + rz_buf[ar, 1, j] + rz_buf[ar, 2, j]
            block = full.at[ar, core, chunks, mine]
            gz.append([
                remote(block, block, sz_sem.at[ar, 1, j0, d], rz_sem.at[ar, 1, j0, d], {"tp": peer})
                for d, peer in enumerate(z_peers)
            ])
            pump(1)
        for i, (j0, j1) in enumerate(GROUPS):
            for d in range(3):
                gz[i][d].wait_recv()
            block = full.at[ar, core, pl.ds(j0, j1 - j0), pl.ds(y * 4, 4)]
            gy.append(remote(block, block, sy_sem.at[ar, 1, j0], ry_sem.at[ar, 1, j0], y_dev))
            pump(1)
        pump(len(pieces))
        for i, (j0, j1) in enumerate(GROUPS):
            gy[i].wait_recv()
            block = full.at[ar, core, pl.ds(j0, j1 - j0)]
            gc.append(remote(block, block, sc_sem.at[ar, 1, j0], rc_sem.at[ar, 1, j0], core_dev))
        for copy in gc:
            copy.wait_recv()
        for copy in cs + ys + gy + gc:
            copy.wait_send()
        for copy in [c for group in zs + gz for c in group]:
            copy.wait_send()

    wo_copy.wait()

    def store_part(j, half, res):
        for r in range(2):
            for u in range(res.shape[1] // LANES):
                part[r, j, half + u] = res[r * HALF:(r + 1) * HALF, u * LANES:(u + 1) * LANES]

    def produce_o(j):
        cols = slice(j * UNITS * LANES, (j + 1) * UNITS * LANES)
        store_part(j, 0, jnp.dot(a_buf[...], wo_buf[:, cols], preferred_element_type=F32))

    all_reduce(0, produce_o, 5)

    sq = [jnp.zeros((HALF, LANES), F32) for _ in range(2)]
    for c in range(width // LANES):
        j, u = divmod(c, UNITS)
        for r in range(2):
            rows, cols = slice(r * HALF, (r + 1) * HALF), slice(c * LANES, (c + 1) * LANES)
            h = (x_ref[rows, cols].astype(F32) + full[0, r, j, u]).astype(BF16)
            h_buf[rows, cols] = h
            hf = h.astype(F32)
            sq[r] = sq[r] + hf * hf
    for r in range(2):
        rows = slice(r * HALF, (r + 1) * HALF)
        inv = lax.rsqrt(jnp.sum(sq[r], axis=-1, keepdims=True) / width + EPS)
        for c in range(width // LANES):
            cols = slice(c * LANES, (c + 1) * LANES)
            n_buf[rows, cols] = (h_buf[rows, cols].astype(F32) * inv * g_ref[cols].astype(F32)[None, :]).astype(BF16)

    pltpu.make_async_copy(wg_hbm, wg_buf, wg_sem).wait()
    pltpu.make_async_copy(wu_hbm, wu_buf, wu_sem).wait()

    def dot_t(a, b):
        return lax.dot_general(a, b, (((1,), (1,)), ((), ())), preferred_element_type=F32)

    def mlp_tile(cols):
        gate = dot_t(n_buf[...], wg_buf[cols, :])
        up = dot_t(n_buf[...], wu_buf[cols, :])
        act[:, cols] = (jax.nn.silu(gate) * up).astype(BF16)

    tiles = ff // 256

    def mlp_step(i, carry):
        mlp_tile(pl.ds(pl.multiple_of(i * 256, 256), 256))
        return carry

    lax.fori_loop(0, tiles, mlp_step, 0)
    if ff % 256:
        mlp_tile(slice(tiles * 256, ff))

    pltpu.make_async_copy(wd_hbm, wd_buf, wd_sem).wait()

    def produce_down(j):
        for half in range(2):
            cols = slice((2 * j + half) * 512, (2 * j + half + 1) * 512)
            store_part(j, half * 4, jnp.dot(act[...], wd_buf[:, cols], preferred_element_type=F32))

    all_reduce(1, produce_down, 2)

    for c in range(width // LANES):
        j, u = divmod(c, UNITS)
        for r in range(2):
            rows, cols = slice(r * HALF, (r + 1) * HALF), slice(c * LANES, (c + 1) * LANES)
            out_ref[rows, cols] = (h_buf[rows, cols].astype(F32) + full[1, r, j, u]).astype(BF16)
    for copy in sends:
        copy.wait_send()


def vmem():
    return pl.BlockSpec(memory_space=pltpu.VMEM)


def anywhere():
    return pl.BlockSpec(memory_space=pl.ANY)


def attention_call(x_in, ctx_len, g_attn, w_qkv, k_cache, v_cache):
    batch, width = x_in.shape
    block, kv_local, head_dim = k_cache.shape[1:]
    cols = w_qkv.shape[1]
    cos_t, sin_t = rope_rows(ctx_len, head_dim)
    flat = (batch, block * kv_local, head_dim)
    dma = pltpu.SemaphoreType.DMA
    acc, ml, k_out, v_out = pl.pallas_call(
        attention_kernel,
        name="attention",
        out_shape=(
            jax.ShapeDtypeStruct((16 * batch, head_dim), F32),
            jax.ShapeDtypeStruct((batch, LANES), F32),
            jax.ShapeDtypeStruct(flat, BF16),
            jax.ShapeDtypeStruct(flat, BF16),
        ),
        in_specs=[pl.BlockSpec(memory_space=pltpu.SMEM)] + [vmem()] * 4 + [anywhere()] * 3,
        out_specs=(vmem(), vmem(), anywhere(), anywhere()),
        scratch_shapes=[
            pltpu.VMEM((width, cols), BF16),
            pltpu.VMEM(flat, BF16),
            pltpu.VMEM(flat, BF16),
            pltpu.VMEM((QKV_STEPS, batch, width // QKV_STEPS), BF16),
            pltpu.VMEM((batch, cols), F32),
            pltpu.VMEM((16 * batch, head_dim), F32),
            pltpu.VMEM((2 * batch, head_dim), F32),
            pltpu.VMEM((2 * batch, head_dim), F32),
            dma((QKV_STEPS,)),
            dma((KV_STEPS,)),
            dma((KV_STEPS,)),
            dma((KV_STEPS,)),
            dma((KV_STEPS,)),
        ],
        compiler_params=pltpu.CompilerParams(vmem_limit_bytes=60 * 1024 * 1024),
        cost_estimate=pl.CostEstimate(flops=2 * batch * width * cols, bytes_accessed=36 << 20, transcendentals=1 << 19),
    )(ctx_len, x_in, g_attn, cos_t, sin_t, w_qkv, k_cache.reshape(flat), v_cache.reshape(flat))
    return acc.reshape(16, batch, head_dim), ml, k_out.reshape(k_cache.shape), v_out.reshape(v_cache.shape)


def tail_call(acc, ml, x_in, g_mlp, w_o, w_gate, w_up, w_down):
    batch, width = x_in.shape
    ff = w_gate.shape[1]
    dma = pltpu.SemaphoreType.DMA
    unit = (HALF, LANES)
    return pl.pallas_call(
        tail_kernel,
        name="tail",
        out_shape=jax.ShapeDtypeStruct((batch, width), BF16),
        in_specs=[vmem()] * 4 + [anywhere()] * 4,
        out_specs=vmem(),
        scratch_shapes=[
            pltpu.VMEM((w_o.shape[0] + 64, width), BF16),
            pltpu.VMEM((ff, width), BF16),
            pltpu.VMEM((ff, width), BF16),
            pltpu.VMEM((ff, width), BF16),
            pltpu.VMEM((3, 3, batch, LANES), F32),
            pltpu.VMEM((3, batch, LANES), F32),
            pltpu.VMEM((batch, 3 * LANES), BF16),
            pltpu.VMEM((2, CHUNKS, UNITS) + unit, F32),
            pltpu.VMEM((2, CHUNKS, UNITS) + unit, F32),
            pltpu.VMEM((2, CHUNKS, 4) + unit, F32),
            pltpu.VMEM((2, 3, CHUNKS) + unit, F32),
            pltpu.VMEM((2, 2, CHUNKS, UNITS) + unit, F32),
            pltpu.VMEM((batch, width), BF16),
            pltpu.VMEM((batch, width), BF16),
            pltpu.VMEM((batch, ff), BF16),
            dma(()), dma(()), dma(()), dma(()),
            dma((3,)), dma((3,)), dma((3,)), dma((3,)),
            dma((2, 2, CHUNKS)), dma((2, 2, CHUNKS)),
            dma((2, 2, CHUNKS)), dma((2, 2, CHUNKS)),
            dma((2, 2, CHUNKS, 3)), dma((2, 2, CHUNKS, 3)),
        ],
        compiler_params=pltpu.CompilerParams(
            collective_id=0, has_side_effects=True, vmem_limit_bytes=67_043_328
        ),
        cost_estimate=pl.CostEstimate(flops=6 * batch * width * ff, bytes_accessed=58 << 20, transcendentals=1 << 17),
    )(acc, ml, x_in, g_mlp, w_o, w_gate.T, w_up.T, w_down)


def solution(mesh):
    x_spec = P("dp", None)
    cache_spec = P("dp", "kvp", "tp", None)
    model_axes = ("tp", "kvp")

    def layer_step(x_in, ctx_len, g_attn, g_mlp, w_qkv, w_o, w_gate, w_up, w_down, k_cache, v_cache):
        acc, ml, k_out, v_out = attention_call(x_in, ctx_len, g_attn, w_qkv, k_cache, v_cache)
        x_out = tail_call(acc, ml, x_in, g_mlp, w_o, w_gate, w_up, w_down)
        return x_out, k_out, v_out

    in_specs = (x_spec, P("dp"), P(None), P(None), P(None, "tp"), P(model_axes, None), P(None, model_axes), P(None, model_axes), P(model_axes, None), cache_spec, cache_spec)
    return jax.shard_map(layer_step, mesh=mesh, in_specs=in_specs, out_specs=(x_spec, cache_spec, cache_spec), check_vma=False)
```
